32 devices in a mesh: row: 8 (over y, x, core), col: 4 (over z).
Axes of the slice: x: 2, y: 2, z: 4, core: 2. Of those that a mesh axis runs over, the one named last changes fastest.
Arguments:
- query: bfloat16 [8, 512, 4096], P(None, 'col'), may hold values from -7 to 7
- key: bfloat16 [4096, 512], P(('row', 'col')), may hold values from -7 to 7
- value: bfloat16 [4096, 512], P(('row', 'col')), may hold values from -4 to 4
- span_order: int32 [32], replicated, may hold values from 0 to 31, each once
Outputs:
- attention: bfloat16 [4096, 4096], P(('row', 'col'))
The draws below stay inside these ranges and needn't reach their ends.
Inputs may be any that keep to these rules, and one draw needn't show every extreme that they name: span_order is a permutation of 0 to 31.
All inputs are finite; a program needn't handle non-finite values.
Results may differ from the reference program's by a relative error of at most 0.0085.
Values may be sent and summed in bfloat16 or wider, within the bound.
No kernel may reach another device: no remote copies, remote signals or barrier semaphores. Data moves between devices by JAX's collectives and lax.ppermute only.
A program may use at most 192 MiB of HBM per device.

```python
import jax
import jax.numpy as jnp
from jax import lax

HEAD_DIM = 128
QHEADS = 32
KVHEADS = 4
TOK_DEV = 128
GROUP_ROWS = 512
SPANS = 32
SEQ = 4096


def draw_pair(key):
    first = jax.random.fold_in(key, 101)
    second = jax.random.fold_in(key, 202)
    key_part = jnp.clip(1.75 * jax.random.normal(first, (SEQ, KVHEADS * HEAD_DIM), jnp.float32), -7.0, 7.0)
    query_part = jnp.clip(1.75 * jax.random.normal(second, (SEQ, QHEADS * HEAD_DIM), jnp.float32), -7.0, 7.0)
    return (query_part, key_part)


def draw_query(key, part):
    query_part, unused = draw_pair(key)
    return query_part.reshape(SEQ // GROUP_ROWS, GROUP_ROWS, QHEADS * HEAD_DIM).astype(jnp.bfloat16)


def draw_key(key, part):
    unused, key_part = draw_pair(key)
    return key_part.astype(jnp.bfloat16)


def shard_levels(stream_key, extent, pieces, smallest, high):
    def one(dim, parts):
        draws = jax.random.uniform(jax.random.fold_in(jax.random.fold_in(stream_key, 6), dim), (parts,), jnp.float32, smallest / len(pieces), high / len(pieces))
        return jnp.repeat(jnp.exp(draws), extent[dim] // parts).reshape((-1,) + (1,) * (len(extent) - dim - 1))

    level = one(*pieces[0])
    for cut in pieces[1:]:
        level = level * one(*cut)
    return level


def scatter_about(rng, dims, scale, bound, shards=(), kind=jnp.bfloat16):
    factor_of = shard_levels(rng, dims, shards, -0.22, 0.18) if shards else 1.0
    array = jax.random.normal(rng, dims, jnp.float32) * scale * factor_of
    return jnp.minimum(jnp.maximum(array, -bound), bound).astype(kind)


def setup_inputs(seed: int = 0) -> dict:
    seeds = jax.random.split(jax.random.key(seed), 5)
    query = draw_query(jax.random.fold_in(seeds[4], 71), 0)
    key = draw_key(jax.random.fold_in(seeds[4], 71), 0)
    value = scatter_about(seeds[2], (SEQ, KVHEADS * HEAD_DIM), 1.0, 4.0, ((0, 32),))
    span_order = jax.random.permutation(seeds[3], SPANS).astype(jnp.int32)
    return dict(query=query, key=key, value=value, span_order=span_order)


masked_score = -1.0e30


def reference(query, key, value, span_order):
    group = QHEADS // KVHEADS
    groups = SEQ // GROUP_ROWS
    offsets = jnp.arange(TOK_DEV, dtype=jnp.int32)
    positions = (span_order.astype(jnp.int32)[:, None] * TOK_DEV + offsets[None, :]).astype(jnp.int32)
    queries = query.reshape(SPANS, TOK_DEV, KVHEADS, group, HEAD_DIM)
    keys = key.reshape(groups, GROUP_ROWS, KVHEADS, HEAD_DIM)
    values = value.reshape(groups, GROUP_ROWS, KVHEADS, HEAD_DIM)
    key_places = positions.reshape(groups, GROUP_ROWS)

    def one_span(inputs):
        span_queries, span_places = inputs
        span_queries = span_queries.astype(jnp.float32)

        def live_group(group_in):
            group_keys, group_values, group_places = group_in
            scores = jnp.einsum("nkgd,skd->nkgs", span_queries, group_keys.astype(jnp.float32)) * (HEAD_DIM ** -0.5)
            visible = group_places[None, None, None, :] <= span_places[:, None, None, None]
            scores = jnp.where(visible, scores, masked_score)
            top = jnp.max(scores, axis=-1)
            raised = jnp.exp(scores - top[..., None])
            total = jnp.sum(raised, axis=-1)
            weights = lax.optimization_barrier(raised.astype(jnp.bfloat16)).astype(jnp.float32)
            summed = jnp.einsum("nkgs,skd->nkgd", weights, group_values.astype(jnp.float32))
            floor = jnp.maximum(total, 1.0)
            partial_value = lax.optimization_barrier((summed / floor[..., None]).astype(jnp.bfloat16)).astype(jnp.float32)
            return partial_value, top + jnp.log(floor)

        def dead_group(group_in):
            partial_value = jnp.zeros((TOK_DEV, KVHEADS, group, HEAD_DIM), span_queries.dtype)
            log_sum = jnp.full((TOK_DEV, KVHEADS, group), masked_score, span_queries.dtype)
            return partial_value, log_sum

        def one_group(group_in):
            group_places = group_in[2]
            alive = jnp.min(group_places) <= jnp.max(span_places)
            return lax.cond(alive, live_group, dead_group, group_in)

        partials, log_sums = lax.map(one_group, (keys, values, key_places))
        highest = jnp.max(log_sums, axis=0)
        combined = highest + jnp.log(jnp.sum(jnp.exp(log_sums - highest), axis=0))
        scale_each = jnp.exp(log_sums - combined)
        merged = jnp.sum(scale_each[..., None] * partials, axis=0)
        return merged.astype(jnp.bfloat16)

    result = lax.map(one_span, (queries, positions))
    return result.reshape(SEQ, QHEADS * HEAD_DIM)
```

```python
import functools
import math

import jax
import jax.numpy as jnp
from jax import lax
from jax.experimental import pallas as pl
from jax.experimental.pallas import tpu as pltpu
from jax.sharding import PartitionSpec as P

HEAD_DIM = 128
QHEADS = 32
KVHEADS = 4
TILE_SPANS = 4

masked_score = -1e30


def attention_kernel(order, ids, query, mine, other, out, keys, values, *, spans, columns, tokens):
    step = pl.program_id(0)
    heads = query.shape[-1] // HEAD_DIM
    half = tokens // 2
    wide = heads * tokens

    @pl.when(step == 0)
    def _():
        parity = ids[2]
        first = pl.multiple_of(parity * half, half)
        second = pl.multiple_of((1 - parity) * half, half)

        def place(span, carry):
            spot = order[span]
            keys[spot, pl.ds(first, half), :] = mine[span, 0]
            keys[spot, pl.ds(second, half), :] = other[span, 0]
            low = jnp.where(parity == 0, mine[span, 1], other[span, 1])
            high = jnp.where(parity == 0, other[span, 1], mine[span, 1])
            whole = jnp.concatenate([low, high], axis=0).astype(jnp.float32)
            values[spot, :HEAD_DIM, :] = whole.T.astype(jnp.bfloat16)
            values[spot, HEAD_DIM:, :] = jnp.ones((16, tokens), jnp.bfloat16)
            return carry

        lax.fori_loop(0, spans, place, 0)

    scaled = query[0].astype(jnp.float32) * (math.log2(math.e) * HEAD_DIM**-0.5)
    turned = jnp.concatenate(
        [scaled[:, h * HEAD_DIM : (h + 1) * HEAD_DIM].T for h in range(heads)], axis=1
    )
    upper = turned.astype(jnp.bfloat16)
    lower = (turned - upper.astype(jnp.float32)).astype(jnp.bfloat16)
    weights = jnp.concatenate([upper, lower], axis=0)

    place = order[step * columns + ids[1]]
    tile = TILE_SPANS * tokens

    def attend(index, state, mask):
        best, summed = state
        block = keys[pl.ds(index * TILE_SPANS, TILE_SPANS)].reshape(tile, HEAD_DIM)
        scores = jnp.dot(
            jnp.concatenate([block, block], axis=1), weights, preferred_element_type=jnp.float32
        )
        if mask:
            row = lax.broadcasted_iota(jnp.int32, (tile, wide), 0) + index * tile
            col = lax.broadcasted_iota(jnp.int32, (tile, wide), 1) % tokens + place * tokens
            scores = jnp.where(row <= col, scores, masked_score)
        newest = jnp.maximum(best, jnp.max(scores, axis=0, keepdims=True))
        shrink = jnp.exp2(best - newest)
        raised = jnp.exp2(scores - newest).astype(jnp.bfloat16)
        block = values[pl.ds(index * TILE_SPANS, TILE_SPANS)]
        block = jnp.concatenate([block[i] for i in range(TILE_SPANS)], axis=1)
        update = jnp.dot(block, raised, preferred_element_type=jnp.float32)
        return newest, summed * shrink + update

    state = (
        jnp.full((1, wide), masked_score, jnp.float32),
        jnp.zeros((HEAD_DIM + 16, wide), jnp.float32),
    )
    whole = place // TILE_SPANS
    state = lax.fori_loop(0, whole, lambda i, s: attend(i, s, False), state)
    best, summed = attend(whole, state, True)
    result = summed[:HEAD_DIM] * (1.0 / summed[HEAD_DIM : HEAD_DIM + 1])
    for h in range(heads):
        out[0, :, h * HEAD_DIM : (h + 1) * HEAD_DIM] = (
            result[:, h * tokens : (h + 1) * tokens].T.astype(jnp.bfloat16)
        )


def shards(query, key, value, span_order):
    rows = lax.axis_size("row")
    columns = lax.axis_size("col")
    row_id = lax.axis_index("row")
    col_id = lax.axis_index("col")
    tokens = key.shape[0]
    spans = rows * columns
    half = tokens // 2
    heads = QHEADS // rows
    sharing = rows // KVHEADS
    width = heads * HEAD_DIM

    pair = jnp.stack([key, value]).reshape(2, 2, half, KVHEADS, HEAD_DIM)
    pair = pair.transpose(3, 1, 0, 2, 4)
    pair = jnp.broadcast_to(
        pair[:, None, :, None], (KVHEADS, sharing // 2, 2, columns, 2, half, HEAD_DIM)
    ).reshape(spans, 2, half, HEAD_DIM)
    mine = lax.all_to_all(pair, ("row", "col"), split_axis=0, concat_axis=0, tiled=True)
    other = lax.ppermute(mine, "row", [(i, i ^ 1) for i in range(rows)])

    ids = jnp.stack([row_id, col_id, row_id % 2]).astype(jnp.int32)
    full = lambda shape: pl.BlockSpec(shape, lambda s, order, ids: (0,) * len(shape))
    result = pl.pallas_call(
        functools.partial(attention_kernel, spans=spans, columns=columns, tokens=tokens),
        grid_spec=pltpu.PrefetchScalarGridSpec(
            num_scalar_prefetch=2,
            grid=(rows,),
            in_specs=[
                pl.BlockSpec((1, tokens, width), lambda s, order, ids: (s, 0, ids[0])),
                full(mine.shape),
                full(other.shape),
            ],
            out_specs=pl.BlockSpec((1, tokens, width), lambda s, order, ids: (s, 0, 0)),
            scratch_shapes=[
                pltpu.VMEM((spans, tokens, HEAD_DIM), jnp.bfloat16),
                pltpu.VMEM((spans, HEAD_DIM + 16, tokens), jnp.bfloat16),
            ],
        ),
        out_shape=jax.ShapeDtypeStruct((rows, tokens, width), jnp.bfloat16),
        compiler_params=pltpu.CompilerParams(vmem_limit_bytes=56 * 2**20),
        name="attention",
    )(span_order, ids, query, mine, other)
    result = lax.all_to_all(result, "row", split_axis=0, concat_axis=0, tiled=True)
    return result.transpose(1, 0, 2).reshape(tokens, rows * width)


def solution(mesh):
    placed = (P(None, "col", None), P(("row", "col"), None), P(("row", "col"), None), P())
    return jax.shard_map(
        shards, mesh=mesh, in_specs=placed, out_specs=P(("row", "col"), None), check_vma=False
    )
```

```python
import functools
import math

import jax
import jax.numpy as jnp
from jax import lax
from jax.experimental import pallas as pl
from jax.experimental.pallas import tpu as pltpu
from jax.sharding import PartitionSpec as P


HEAD_DIM = 128
QHEADS = 32
KVHEADS = 4
TILE_SPANS = 2
EXTRA = 16

masked_score = -1e30


def attention_kernel(*refs, pieces, first, last, tokens):
    refs = list(refs)
    meta = refs.pop(0)
    blocks = [refs.pop(0) for _ in range(pieces)]
    if first:
        query = refs.pop(0)
    else:
        qt_in, best_in, acc_in = (refs.pop(0) for _ in range(3))
    if last:
        out = refs.pop(0)
    else:
        qt_out, best_out, acc_out = (refs.pop(0) for _ in range(3))
    keys, values, best, acc, s0, s1, p0, p1, items = refs[:9]
    qt = qt_out if first and not last else (refs[9] if first else qt_in)
    steps, _, wide = qt.shape
    heads = wide // HEAD_DIM
    spans = sum(block.shape[0] for block in blocks)
    per = blocks[0].shape[0]
    tile = TILE_SPANS * tokens

    for index, block in enumerate(blocks):
        def place(span, carry, block=block, index=index):
            spot = meta[index * per + span]
            keys[spot] = block[span, 0]
            values[spot, :HEAD_DIM] = block[span, 1].astype(jnp.float32).T.astype(jnp.bfloat16)
            values[spot, HEAD_DIM:] = jnp.ones((EXTRA, tokens), jnp.bfloat16)
            return carry

        lax.fori_loop(0, per, place, 0, unroll=4)

    def count(s):
        return meta[spans + s]

    if first:
        def turn(s, carry):
            scaled = query[s].astype(jnp.float32) * (math.log2(math.e) * HEAD_DIM**-0.5)
            for h in range(heads):
                lanes = slice(h * HEAD_DIM, (h + 1) * HEAD_DIM)
                turned = scaled[:, lanes].T
                upper = turned.astype(jnp.bfloat16)
                qt[s, :HEAD_DIM, lanes] = upper
                qt[s, HEAD_DIM:, lanes] = (turned - upper.astype(jnp.float32)).astype(jnp.bfloat16)
            return carry

        lax.fori_loop(0, steps, turn, 0, unroll=2)

        row = lax.broadcasted_iota(jnp.int32, (tokens, wide), 0)
        col = lax.broadcasted_iota(jnp.int32, (tokens, wide), 1) % tokens
        seen = row <= col

        def diagonal(pair, carry):
            for s in (pair * 2, pair * 2 + 1):
                spot = count(s)
                block = keys[spot]
                scores = jnp.dot(
                    jnp.concatenate([block, block], axis=1), qt[s], preferred_element_type=jnp.float32
                )
                scores = jnp.where(seen, scores, masked_score)
                top = jnp.max(scores, axis=0, keepdims=True)
                raised = jnp.exp2(scores - top).astype(jnp.bfloat16)
                best[s] = top
                acc[s] = jnp.dot(values[spot], raised, preferred_element_type=jnp.float32)
            return carry

        lax.fori_loop(0, steps // 2, diagonal, 0)
    else:
        def load(s, carry):
            best[s] = best_in[s]
            acc[s] = acc_in[s]
            return carry

        lax.fori_loop(0, steps, load, 0)
    best[steps] = jnp.zeros((1, wide), jnp.float32)
    acc[steps] = jnp.zeros(acc.shape[1:], jnp.float32)
    p1[...] = jnp.zeros(p1.shape, p1.dtype)

    idle = steps * 256
    items[0] = idle

    def list_span(s, n):
        def one(t, n):
            items[n] = s * 256 + t
            return n + 1

        return lax.fori_loop(0, lax.div(count(s) + (TILE_SPANS - 1), jnp.int32(TILE_SPANS)), one, n)

    n = lax.fori_loop(0, steps, list_span, 1)
    for k in range(4):
        items[n + k] = idle

    def split(i):
        item = items[i]
        return item >> 8, item & 255

    def score(i, target):
        s, t = split(i)
        block = keys[pl.ds(t * TILE_SPANS, TILE_SPANS)].reshape(tile, HEAD_DIM)
        scores = jnp.dot(
            jnp.concatenate([block, block], axis=1),
            qt[jnp.minimum(s, steps - 1)],
            preferred_element_type=jnp.float32,
        )
        target[...] = scores
        return [
            jnp.max(scores[j * tokens : (j + 1) * tokens], axis=0, keepdims=True)
            for j in range(TILE_SPANS)
        ]

    def soften(i, tops, source, target):
        s, t = split(i)
        left = jnp.where(s < steps, count(jnp.minimum(s, steps - 1)), 0) - t * TILE_SPANS
        old = best[s]
        new = old
        for j in range(TILE_SPANS):
            new = jnp.maximum(new, jnp.where(j < left, tops[j], masked_score))
        best[s] = new
        for j in range(TILE_SPANS):
            rows = slice(j * tokens, (j + 1) * tokens)
            base = jnp.where(j < left, new, -masked_score)
            target[rows] = jnp.exp2(source[rows] - base).astype(jnp.bfloat16)
        return jnp.exp2(old - new)

    def gather(i, shrink, source):
        s, t = split(i)
        block = values[pl.ds(t * TILE_SPANS, TILE_SPANS)]
        block = jnp.concatenate([block[j] for j in range(TILE_SPANS)], axis=1)
        acc[s] = acc[s] * shrink + jnp.dot(block, source[...], preferred_element_type=jnp.float32)

    def body(k, carry):
        tops, shrink = carry
        i = 1 + 2 * k
        tops_b = score(i + 1, s1)
        shrink_b = soften(i, tops, s0, p0)
        gather(i - 1, shrink, p1)
        tops_c = score(i + 2, s0)
        shrink_c = soften(i + 1, tops_b, s1, p1)
        gather(i, shrink_b, p0)
        return tops_c, shrink_c

    lax.fori_loop(0, (n + 1) >> 1, body, (score(1, s0), jnp.ones((1, wide), jnp.float32)))

    def finish(s, carry):
        if last:
            total = acc[s]
            result = total[:HEAD_DIM] * (1.0 / total[HEAD_DIM : HEAD_DIM + 1])
            for h in range(heads):
                lanes = slice(h * HEAD_DIM, (h + 1) * HEAD_DIM)
                out[s, :, lanes] = result[:, h * tokens : (h + 1) * tokens].T.astype(jnp.bfloat16)
        else:
            best_out[s] = best[s]
            acc_out[s] = acc[s]
            if not first:
                qt_out[s] = qt_in[s]
        return carry

    lax.fori_loop(0, steps, finish, 0, unroll=2)


def attend(meta, blocks, query, state, last, steps, tokens, width):
    first = query is not None
    spans = sum(block.shape[0] for block in blocks)
    room = -(-spans // TILE_SPANS) * TILE_SPANS
    tile = TILE_SPANS * tokens
    vmem = pl.BlockSpec(memory_space=pltpu.VMEM)
    operands = [*blocks, query] if first else [*blocks, *state]
    if last:
        shapes = [jax.ShapeDtypeStruct((steps, tokens, width), jnp.bfloat16)]
    else:
        shapes = [
            jax.ShapeDtypeStruct((steps, 2 * HEAD_DIM, width), jnp.bfloat16),
            jax.ShapeDtypeStruct((steps, 1, width), jnp.float32),
            jax.ShapeDtypeStruct((steps, HEAD_DIM + EXTRA, width), jnp.float32),
        ]
    scratch = [
        pltpu.VMEM((room, tokens, HEAD_DIM), jnp.bfloat16),
        pltpu.VMEM((room, HEAD_DIM + EXTRA, tokens), jnp.bfloat16),
        pltpu.VMEM((steps + 1, 1, width), jnp.float32),
        pltpu.VMEM((steps + 1, HEAD_DIM + EXTRA, width), jnp.float32),
        pltpu.VMEM((tile, width), jnp.float32),
        pltpu.VMEM((tile, width), jnp.float32),
        pltpu.VMEM((tile, width), jnp.bfloat16),
        pltpu.VMEM((tile, width), jnp.bfloat16),
        pltpu.SMEM((steps * (room // TILE_SPANS) + 8,), jnp.int32),
    ]
    if first and last:
        scratch.append(pltpu.VMEM((steps, 2 * HEAD_DIM, width), jnp.bfloat16))
    work = steps * spans * tokens * tokens * width * 2
    return pl.pallas_call(
        functools.partial(
            attention_kernel, pieces=len(blocks), first=first, last=last, tokens=tokens
        ),
        in_specs=[pl.BlockSpec(memory_space=pltpu.SMEM)] + [vmem] * len(operands),
        out_specs=[vmem] * len(shapes),
        out_shape=shapes,
        scratch_shapes=scratch,
        cost_estimate=pl.CostEstimate(
            flops=work, bytes_accessed=8 * 2**20, transcendentals=work // (4 * HEAD_DIM)
        ),
        compiler_params=pltpu.CompilerParams(vmem_limit_bytes=40 * 2**20),
        name="attention",
    )(meta, *operands)


def lookup(table, indices):
    columns = jnp.arange(table.shape[0], dtype=jnp.int32)
    chosen = jnp.where(indices[:, None] == columns[None, :], table[None, :], 0)
    return jnp.sum(chosen, axis=1)


def shards(query, key, value, span_order):
    rows = lax.axis_size("row")
    columns = lax.axis_size("col")
    row_id = lax.axis_index("row")
    col_id = lax.axis_index("col")
    tokens = key.shape[0]
    heads = QHEADS // rows
    sharing = rows // KVHEADS
    width = heads * HEAD_DIM
    deltas = list(range(0, rows, 2))

    def piece(row):
        start = lax.div(row, jnp.int32(sharing)) * HEAD_DIM
        return jnp.stack([lax.dynamic_slice_in_dim(x, start, HEAD_DIM, 1) for x in (key, value)])

    parts = [piece(row_id)]
    for delta in deltas[1:]:
        pairs = [(i, i ^ delta) for i in range(rows)]
        parts.append(lax.ppermute(piece(row_id ^ delta), "row", pairs))
    own = jnp.stack(parts)

    across = [(i, i ^ 1) for i in range(rows)]
    mine = [own]
    for s in range(1, columns):
        pairs = [(i, (i + s) % columns) for i in range(columns)]
        mine.append(lax.ppermute(own, "col", pairs))
    query_orders = lookup(span_order, jnp.arange(rows, dtype=jnp.int32) * columns + col_id)
    near = row_id ^ jnp.array(deltas, jnp.int32)
    taken = lax.dynamic_slice_in_dim(query, row_id * width, width, 2)

    def describe(shift):
        source = lax.rem(col_id + (columns - shift), jnp.int32(columns))
        held = jnp.concatenate([near, near ^ 1]) * columns + source
        orders = lookup(span_order, held)
        rank = jnp.sum(orders[None, :] < orders[:, None], axis=1)
        count = jnp.sum(orders[None, :] < query_orders[:, None], axis=1)
        return jnp.concatenate([rank, count]).astype(jnp.int32)

    state = None
    for shift, block in enumerate(mine):
        if state is not None:
            block, tops = lax.optimization_barrier((block, state[1]))
            state = [state[0], tops, state[2]]
        meta = describe(shift)
        other = lax.ppermute(block, "row", across)
        state = attend(
            meta,
            [block, other],
            taken if shift == 0 else None,
            state,
            shift == columns - 1,
            rows,
            tokens,
            width,
        )
    result = lax.all_to_all(state[0], "row", split_axis=0, concat_axis=0, tiled=True)
    return result.transpose(1, 0, 2).reshape(tokens, rows * width)


def solution(mesh):
    placed = (P(None, "col", None), P(("row", "col"), None), P(("row", "col"), None), P())

    return jax.shard_map(
        shards, mesh=mesh, in_specs=placed, out_specs=P(("row", "col"), None), check_vma=False
    )
```
